512 devices in a mesh: runner: 16 (over z), cells: 32 (over x, y, core).
Axes of the slice: x: 4, y: 4, z: 16, core: 2. Of those that a mesh axis runs over, the one named last changes fastest.
Arguments:
- states: float32 [2048, 256, 128], P('runner', 'cells'), may hold values from -4 to 4
- diffusivity: float32 [256, 128], P('cells'), may hold values from 0.03 to 0.2
- velocity: float32 [2, 256, 128], P(None, 'cells'), may hold values from -0.15 to 0.15
- counts: int32 [16], replicated, may hold values from 1 to 128, 1024 in all
- obs_index: int32 [16384], P('cells'), may hold values from 0 to 1023
- obs_value: float32 [16384], P('cells'), may hold values from -6 to 6
- obs_weight: float32 [16384], P('cells'), may hold values from 0.3 to 3
Outputs:
- analysed: float32 [2048, 256, 128], P('runner', 'cells')
The draws below stay inside these ranges and needn't reach their ends.
Inputs may be any that keep to these rules, and one draw needn't show every extreme that they name: Runner r's members fill its first counts[r] slots, in runner order; the counts sum to 1024 and the largest is exactly 128. Observation k lies in the rows of cells index k // 512; obs_index counts cells within those 8 x 128 cells, row by row; a cell may be observed more than once.
All inputs are finite; a program needn't handle non-finite values.
Results may differ from the reference program's by a relative error of at most 0.013.
Values may be sent and summed in bfloat16 or wider, within the bound.
A program may use at most 64 MiB of HBM per device.

```python
import math
import jax
import jax.numpy as jnp
import numpy as np
from jax import lax

CX = 8
GRID_COLUMNS = 128
OBS_DEV = 512
STEPS = 4
RUNNER_SLOTS = 128
MEMBER_COUNT = 1024
GRID_ROWS = 256
NOBS = 16384
N_RUNNER = 16


def with_ends(result, stream_key, low, top_value):
    shape = result.shape
    index_at = [jax.random.randint(jax.random.fold_in(stream_key, axis), (), 0, shape[axis]) for axis in range(len(shape))]
    result = result.at[tuple(index_at)].set(low)
    longest = shape.index(max(shape))
    index_at[longest] = (index_at[longest] + 1) % shape[longest]
    return result.at[tuple(index_at)].set(top_value)


def block_scale(own_key, extent, split, smallest, high):
    loudness = 1.0
    for dim, shards_of in split:
        draws = jax.random.uniform(jax.random.fold_in(jax.random.fold_in(own_key, 6), dim), (shards_of,), jnp.float32, smallest / len(split), high / len(split))
        loudness = loudness * jnp.repeat(jnp.exp(draws), extent[dim] // shards_of).reshape((-1,) + (1,) * (len(extent) - 1 - dim))
    return loudness


def split_up(count, total, bound, lean):
    loads = [(1 << 20) // math.isqrt(standing ** lean) + 1 for standing in range(2, count + 1)]
    rest, given = total - bound - (count - 1), [1] * (count - 1)
    while rest > 0:
        movable = [i for i in range(count - 1) if given[i] < bound]
        pool, budget = sum([loads[i] for i in movable]), rest
        for i in movable:
            extra = min(bound - given[i], max(1, budget * loads[i] // pool), rest)
            given[i] = given[i] + extra
            rest = rest - extra
    return np.array([bound] + given)


def ragged_sizes(rng, number_of, total, limit, lean):
    if number_of == 2:
        one = jax.random.randint(rng, (), max(1, total - limit), min(limit, total - 1) + 1)
        return jnp.stack([one, total - one])
    lengths = jnp.asarray(split_up(number_of, total, limit, lean), jnp.int32)
    pairs = (number_of - 1) // 2
    giver, receiver = lengths[1:1 + 2 * pairs:2], lengths[2:2 + 2 * pairs:2]
    room = jnp.minimum(giver - 1, limit - receiver)
    moved = jax.random.randint(jax.random.fold_in(rng, 1), (pairs,), 0, 1 << 20) % (room + 1)
    lengths = lengths.at[1:1 + 2 * pairs:2].set(giver - moved).at[2:2 + 2 * pairs:2].set(receiver + moved)
    return lengths[jax.random.permutation(jax.random.fold_in(rng, 2), number_of)]


def gaussian(key, extent, spread, reach, shards=(), kind=jnp.bfloat16):
    entries = spread * jax.random.normal(key, extent, jnp.float32)
    if shards:
        entries = entries * block_scale(key, extent, shards, -0.22, 0.18)
    return jnp.clip(entries, -reach, reach).astype(kind)


def setup_inputs(seed: int = 0) -> dict:
    seeds = jax.random.split(jax.random.key(seed), 8)
    states = gaussian(seeds[0], (N_RUNNER * RUNNER_SLOTS, GRID_ROWS, GRID_COLUMNS), 0.7, 4.0, ((0, 16), (1, 32)), jnp.float32)
    diffusivity = jnp.clip(jnp.exp(math.log(0.2) - 1.89712 * jax.random.uniform(seeds[1], (GRID_ROWS, GRID_COLUMNS), jnp.float32) ** block_scale(seeds[1], (GRID_ROWS, GRID_COLUMNS), ((0, 32),), -0.2, 0.2)), 0.03, 0.2)
    velocity = jnp.clip(jax.random.uniform(seeds[2], (2, GRID_ROWS, GRID_COLUMNS), jnp.float32, -0.15, 0.15) * block_scale(seeds[2], (2, GRID_ROWS, GRID_COLUMNS), ((1, 32),), -0.4, 0.0), -0.15, 0.15)
    counts = ragged_sizes(seeds[3], N_RUNNER, MEMBER_COUNT, RUNNER_SLOTS, 2).astype(jnp.int32)
    obs_index = with_ends(jax.random.randint(seeds[4], (NOBS,), 0, CX * GRID_COLUMNS), jax.random.fold_in(seeds[4], 1), 0, (CX * GRID_COLUMNS) - 1).astype(jnp.int32)
    obs_value = gaussian(seeds[5], (NOBS,), 1.0, 6.0, ((0, 32),), jnp.float32)
    obs_weight = jnp.clip(jnp.exp(math.log(3.0) - 2.3025851 * jax.random.uniform(seeds[6], (NOBS,), jnp.float32) ** block_scale(seeds[6], (NOBS,), ((0, 32),), -0.2, 0.2)), 0.3, 3.0)
    return {"states": states, "diffusivity": diffusivity, "velocity": velocity, "counts": counts, "obs_index": obs_index, "obs_value": obs_value, "obs_weight": obs_weight}


def stencil(values, diffusivity, velocity):
    upper_row = jnp.roll(values, -1, axis=-2)
    lower_row = jnp.roll(values, 1, axis=-2)
    right_col = jnp.roll(values, -1, axis=-1)
    left_col = jnp.roll(values, 1, axis=-1)
    laplace = upper_row + lower_row + right_col + left_col - 4.0 * values
    return (values + diffusivity * laplace - 0.5 * velocity[0] * (upper_row - lower_row)
            - 0.5 * velocity[1] * (right_col - left_col) - 0.05 * values * values * values)


def reference(states, diffusivity, velocity, counts, obs_index, obs_value, obs_weight):
    worker_blocks = states.reshape(N_RUNNER, RUNNER_SLOTS, GRID_ROWS, GRID_COLUMNS)

    def march_forward(block_states):
        values = block_states
        for iteration in range(STEPS):
            values = stencil(values, diffusivity, velocity)
        return values

    predicted_states = lax.map(march_forward, worker_blocks).reshape(N_RUNNER * RUNNER_SLOTS, GRID_ROWS * GRID_COLUMNS)
    run_ends = jnp.cumsum(counts).astype(jnp.int32)
    offsets = (run_ends - counts).astype(jnp.int32)
    slot_ids = jnp.arange(RUNNER_SLOTS, dtype=jnp.int32)
    is_live = (slot_ids[None, :] < counts[:, None]).reshape(-1)
    member_ids = jnp.arange(MEMBER_COUNT, dtype=jnp.int32)
    owner_run = jnp.sum((run_ends[None, :] <= member_ids[:, None]).astype(jnp.int32), axis=1).astype(jnp.int32)
    slot_of = (owner_run * RUNNER_SLOTS + member_ids - offsets[owner_run]).astype(jnp.int32)
    active_mask = is_live.astype(jnp.float32)[:, None]
    ensemble_mean = jnp.sum(predicted_states * active_mask, axis=0) / MEMBER_COUNT
    member_deviation = ((predicted_states - ensemble_mean) * active_mask).astype(jnp.bfloat16)
    compact = member_deviation[slot_of]
    obs_cells = ((jnp.arange(NOBS, dtype=jnp.int32) // OBS_DEV) * (CX * GRID_COLUMNS) + obs_index).astype(jnp.int32)
    observed = compact[:, obs_cells]
    weighted = (observed.astype(jnp.float32) * obs_weight).astype(jnp.bfloat16)
    gram_full = jnp.dot(weighted, observed.T, preferred_element_type=jnp.float32)
    trace_sum = jnp.trace(gram_full)
    scaling = MEMBER_COUNT / trace_sum
    innovation = obs_value - ensemble_mean[obs_cells]
    bias_vector = (jnp.dot(weighted.astype(jnp.float32), innovation, precision=lax.Precision.HIGHEST) * scaling).astype(jnp.bfloat16)
    scaled = (gram_full * scaling).astype(jnp.bfloat16)
    square = jnp.dot(scaled, scaled, preferred_element_type=jnp.float32).astype(jnp.bfloat16)
    cubed = jnp.dot(square, scaled, preferred_element_type=jnp.float32)
    transform = (1.0 * jnp.eye(MEMBER_COUNT, dtype=jnp.float32) - 0.5 * scaled.astype(jnp.float32)
                 + 0.375 * square.astype(jnp.float32) - 0.3125 * cubed)
    shift_weights = jnp.dot(transform, bias_vector.astype(jnp.float32), precision=lax.Precision.HIGHEST)
    increment = jnp.dot(shift_weights, compact.astype(jnp.float32), precision=lax.Precision.HIGHEST)
    applied = jnp.dot(transform.astype(jnp.bfloat16), compact, preferred_element_type=jnp.float32)
    analysed = ensemble_mean + increment + applied
    slotted = jnp.zeros((N_RUNNER * RUNNER_SLOTS, GRID_ROWS * GRID_COLUMNS), jnp.float32).at[slot_of].set(analysed)
    return slotted.reshape(N_RUNNER * RUNNER_SLOTS, GRID_ROWS, GRID_COLUMNS)
```

```python
import functools

import jax
import jax.numpy as jnp
from jax import lax
from jax.experimental import pallas as pl
from jax.experimental.pallas import tpu as pltpu
from jax.sharding import PartitionSpec as P

MESH = pl.DeviceIdType.MESH
STEPS = 4
F32 = jnp.float32
BF16 = jnp.bfloat16
VMEM = pltpu.VMEM
DMA = pltpu.SemaphoreType.DMA


def split3(x):
    hi = x.astype(BF16)
    rest = x - hi.astype(F32)
    mid = rest.astype(BF16)
    low = (rest - mid.astype(F32)).astype(BF16)
    return hi, mid, low


def rows_of(parts, rows):
    have = sum(p.shape[0] for p in parts)
    if have < rows:
        parts = list(parts) + [jnp.zeros((rows - have, parts[0].shape[1]), parts[0].dtype)]
    return jnp.concatenate(parts, axis=0)


def dot(a, b):
    return lax.dot_general(a, b, (((1,), (0,)), ((), ())), preferred_element_type=F32)


def dot_t(a, b):
    return lax.dot_general(a, b, (((1,), (1,)), ((), ())), preferred_element_type=F32)


def halo_kernel(cells, st, fl, prev_out, next_out, fprev_out, fnext_out, hi_s, lo_s, fhi_s, flo_s, ssem, rsem):
    me = lax.axis_index("cells")
    nxt = lax.rem(me + 1, cells)
    prv = lax.rem(me + cells - 1, cells)
    barrier = pltpu.get_barrier_semaphore()
    for who in (nxt, prv):
        pl.semaphore_signal(barrier, inc=1, device_id={"cells": who}, device_id_type=MESH)
    width = st.shape[2]
    rows = st.shape[1]
    for k in range(STEPS):
        cols = slice(k * width, (k + 1) * width)
        lo_s[:, cols] = st[:, k, :].astype(BF16)
        hi_s[:, cols] = st[:, rows - STEPS + k, :].astype(BF16)
    for f in range(3):
        flo_s[f] = fl[f, 0:STEPS, :]
        fhi_s[f] = fl[f, rows - STEPS : rows, :]
    pl.semaphore_wait(barrier, 2)
    copies = []
    for n, (src, dst, who) in enumerate(
        ((hi_s, prev_out, nxt), (lo_s, next_out, prv), (fhi_s, fprev_out, nxt), (flo_s, fnext_out, prv))
    ):
        copies.append(
            pltpu.make_async_remote_copy(
                src_ref=src, dst_ref=dst, send_sem=ssem.at[n], recv_sem=rsem.at[n],
                device_id={"cells": who}, device_id_type=MESH,
            )
        )
    for copy in copies:
        copy.start()
    for copy in copies:
        copy.wait()


def main_kernel(
    R, C,
    st, hprev, hnext, fl, fprev, fnext, counts, obs_idx, obs_val, obs_w,
    out,
    cf, fc, offs, qt, pt, abuf, ap, lmb, gp, rsb, bsb, brow, gs, sz, sb,
    lm_s, lm_r, ring_s, ring_r, rs_s, rs_r, b_s, b_r, z_s, z_r, pl_s, pl_r, rl_s, rl_r,
):
    SL, X, Y = st.shape
    CELLS = X * Y
    M = SL // 2 * R
    PAD = SL * R
    H = CELLS // 2
    NJ = C // 4
    HALF = R // 2
    NCH = C // 2
    OBS = obs_idx.shape[1]
    me = lax.axis_index("runner")
    mec = lax.axis_index("cells")
    core = lax.rem(mec, 2)
    chip = mec // 2

    barrier = pltpu.get_barrier_semaphore()

    def greet_z(d, _):
        pl.semaphore_signal(barrier, inc=1, device_id={"runner": lax.rem(me + d, R)}, device_id_type=MESH)
        return 0

    def greet_c(d, _):
        pl.semaphore_signal(barrier, inc=1, device_id={"cells": lax.rem(mec + d, C)}, device_id_type=MESH)
        return 0

    lax.fori_loop(1, R, greet_z, 0)
    lax.fori_loop(1, C, greet_c, 0)

    total = jnp.int32(0)
    for q in range(R):
        offs[q] = total
        total = total + counts[q]
    own = counts[me]

    for k in range(X + 2 * STEPS):
        if k < STEPS:
            d, v0, v1 = (fprev[f, k : k + 1, :] for f in range(3))
        elif k < STEPS + X:
            d, v0, v1 = (fl[f, k - STEPS : k - STEPS + 1, :] for f in range(3))
        else:
            d, v0, v1 = (fnext[f, k - STEPS - X : k - STEPS - X + 1, :] for f in range(3))
        cf[0, k : k + 1, :] = d - 0.5 * v0
        cf[1, k : k + 1, :] = d + 0.5 * v0
        cf[2, k : k + 1, :] = d - 0.5 * v1
        cf[3, k : k + 1, :] = d + 0.5 * v1
        cf[4, k : k + 1, :] = 1.0 - 4.0 * d

    def march(g, _):
        sl = pl.ds(pl.multiple_of(g * 16, 16), 16)
        u = [hprev[sl, k * Y : (k + 1) * Y].astype(F32) for k in range(STEPS)]
        u += [st[sl, k, :] for k in range(X)]
        u += [hnext[sl, k * Y : (k + 1) * Y].astype(F32) for k in range(STEPS)]
        for step in range(STEPS):
            new = []
            for k in range(1, len(u) - 1):
                row = k + step
                c = u[k]
                right = pltpu.roll(c, Y - 1, 1)
                left = pltpu.roll(c, 1, 1)
                acc = cf[0, row : row + 1, :] * u[k + 1] + cf[1, row : row + 1, :] * u[k - 1]
                acc = acc + cf[2, row : row + 1, :] * right + cf[3, row : row + 1, :] * left
                acc = acc + c * (cf[4, row : row + 1, :] - 0.05 * (c * c))
                new.append(acc)
            u = new
        for k in range(X):
            fc[sl, k * Y : (k + 1) * Y] = u[k]
        return 0

    lax.fori_loop(0, SL // 16, march, 0)

    slot = lax.broadcasted_iota(jnp.int32, (SL, 1), 0)
    live = slot < own
    lsum = jnp.sum(jnp.where(live, fc[...], 0.0), axis=0, keepdims=True)
    lmean = lsum / own.astype(F32)
    local = jnp.where(live, fc[...] - lmean, 0.0).astype(BF16)

    cell_c = lax.broadcasted_iota(jnp.int32, (CELLS, OBS), 0)
    hot = jnp.where(cell_c == obs_idx[...], 1.0, 0.0).astype(BF16)
    w = obs_w[...]
    ones = jnp.ones((1, OBS), BF16)
    x = rows_of([ones, *split3(w), *split3(w * obs_val[...])], 16)
    sums = dot_t(x, hot)
    flag = sums[0:1] > 0.5
    wsum = sums[1:2] + sums[2:3] + sums[3:4]
    vsum = sums[4:5] + sums[5:6] + sums[6:7]
    r_i = lax.broadcasted_iota(jnp.int32, (CELLS, CELLS), 0)
    c_i = lax.broadcasted_iota(jnp.int32, (CELLS, CELLS), 1)
    upper = jnp.where(r_i < c_i, 1.0, 0.0).astype(BF16)
    flags = jnp.where(flag, 1.0, 0.0)
    before = dot(rows_of([flags.astype(BF16)], 16), upper)[0:1]
    n_obs = jnp.sum(flags, axis=1, keepdims=True)
    cell_r = lax.broadcasted_iota(jnp.int32, (1, CELLS), 1).astype(F32)
    place = jnp.where(flag, before, n_obs + cell_r - before).astype(jnp.int32)
    pt[...] = jnp.where(r_i == place, 1.0, 0.0).astype(BF16)

    moved = dot_t(local, pt[...]).astype(BF16)
    rows3 = rows_of([*split3(lmean), *split3(wsum), *split3(vsum)], 16)
    rows3 = dot_t(rows3, pt[...])
    lmb[me] = rows3[0:1] + rows3[1:2] + rows3[2:3]
    wperm = (rows3[3:4] + rows3[4:5] + rows3[5:6])[:, :H]
    vperm = (rows3[6:7] + rows3[7:8] + rows3[8:9])[:, :H]
    abuf[me, 0] = moved[:, :H]
    abuf[me, 1] = moved[:, H:]

    pl.semaphore_wait(barrier, R + C - 2)

    def lm_copy(d):
        return pltpu.make_async_remote_copy(
            src_ref=lmb.at[me], dst_ref=lmb.at[me], send_sem=lm_s.at[d], recv_sem=lm_r.at[d],
            device_id={"runner": lax.rem(me + d, R)}, device_id_type=MESH,
        )

    def start_lm(d, _):
        lm_copy(d).start()
        return 0

    def wait_lm(d, _):
        lm_copy(d).wait()
        return 0

    SUB = SL // 2

    def ring_copy(h, s, way, sub):
        owner = lax.rem(me - s + R, R) if way == 0 else lax.rem(me + s, R)
        to = lax.rem(me + 1, R) if way == 0 else lax.rem(me + R - 1, R)
        part = abuf.at[owner, h, pl.ds(sub * SUB, SUB)]
        return pltpu.make_async_remote_copy(
            src_ref=part, dst_ref=part,
            send_sem=ring_s.at[way, h, s, sub], recv_sem=ring_r.at[way, h, s, sub],
            device_id={"runner": to}, device_id_type=MESH,
        )

    pieces = [(0, 0), (1, 1), (0, 1), (1, 0)]
    last_pieces = [(0, 0), (1, 1)]

    def ring_start(h):
        for way, sub in pieces if HALF > 1 else last_pieces:
            ring_copy(h, 0, way, sub).start()

    def ring_step(h, s, last=False, before_last=False):
        for way, sub in last_pieces if last else pieces:
            ring_copy(h, s, way, sub).wait_recv()
            if not last and (not before_last or (way, sub) in last_pieces):
                ring_copy(h, s + 1, way, sub).start()

    def ring_sent(h):
        def sent(s, _):
            for way, sub in pieces:
                ring_copy(h, s, way, sub).wait_send()
            return 0

        lax.fori_loop(0, HALF - 1, sent, 0)
        for way, sub in last_pieces:
            ring_copy(h, HALF - 1, way, sub).wait_send()

    ring_start(0)
    lax.fori_loop(1, R, start_lm, 0)

    slots = lax.broadcasted_iota(jnp.int32, (SL, M), 0)
    mems = lax.broadcasted_iota(jnp.int32, (SL, M), 1)

    def build(q, _):
        hit = (mems == slots + offs[q]) & (slots < counts[q])
        qt[pl.ds(pl.multiple_of(q * SL, SL), SL), :] = jnp.where(hit, 1.0, 0.0).astype(BF16)
        return 0

    lax.fori_loop(0, R, build, 0)
    p_i = lax.broadcasted_iota(jnp.int32, (64, SL), 0)
    l_i = lax.broadcasted_iota(jnp.int32, (64, SL), 1)
    wanted = (p_i >> 4) * (16 * R) + 16 * me + (p_i & 15)
    pick = []
    for q in range(R):
        hit = (wanted == l_i + offs[q]) & (l_i < counts[q])
        pick.append(jnp.where(hit, 1.0, 0.0).astype(BF16))
    pick = jnp.concatenate(pick, axis=1)

    lax.fori_loop(1, R, wait_lm, 0)
    mean = jnp.zeros((1, CELLS), F32)
    for q in range(R):
        mean = mean + counts[q].astype(F32) * lmb[q]
    mean = mean / M

    def centre(h, q):
        shift = (lmb[q] - mean)[:, h * H : (h + 1) * H]
        value = abuf[q, h].astype(F32) + shift
        ap[h, pl.ds(pl.multiple_of(q * SL, SL), SL), :] = jnp.where(slot < counts[q], value, 0.0).astype(BF16)

    def run_ring(h, first, last):
        def one(s, _):
            ring_step(h, s)
            centre(h, lax.rem(me - 1 - s + 2 * R, R))
            centre(h, lax.rem(me + 1 + s, R))
            return 0

        if last > first:
            lax.fori_loop(first, last, one, 0)

    def end_ring(h):
        if HALF > 1:
            ring_step(h, HALF - 2, before_last=True)
            centre(h, lax.rem(me - 1 - (HALF - 2) + 2 * R, R))
            centre(h, lax.rem(me + 1 + (HALF - 2), R))

    def finish_ring(h):
        ring_step(h, HALF - 1, last=True)
        centre(h, lax.rem(me + HALF, R))

    centre(0, me)
    run_ring(0, 0, HALF - 2)
    end_ring(0)
    ring_start(1)
    finish_ring(0)

    rows_a = dot(pick, ap[0])
    weighted = (rows_a * wperm).astype(BF16)
    grad = vperm - wperm * mean[:, :H]
    left = jnp.concatenate([weighted, rows_of(list(split3(grad)), 16)], axis=0)
    wide = dot_t(left, ap[0])
    wide_hi = wide.astype(BF16)
    wide_lo = (wide - wide_hi.astype(F32)).astype(BF16)
    both = dot(jnp.concatenate([wide_hi, wide_lo], axis=0), qt[...])
    gram = both[0:80] + both[80:160]
    for c in range(C):
        i, j = c // NJ, c % NJ
        gp[c] = gram[16 * i : 16 * i + 16, 128 * j : 128 * j + 128].astype(BF16)
    bsb[mec] = gram[64:65] + gram[65:66] + gram[66:67]

    def rs_copy(d):
        to = lax.rem(mec + d, C)
        return pltpu.make_async_remote_copy(
            src_ref=gp.at[to], dst_ref=rsb.at[mec], send_sem=rs_s.at[d], recv_sem=rs_r.at[d],
            device_id={"cells": to}, device_id_type=MESH,
        )

    def b_copy(d):
        return pltpu.make_async_remote_copy(
            src_ref=bsb.at[mec], dst_ref=bsb.at[mec], send_sem=b_s.at[d], recv_sem=b_r.at[d],
            device_id={"cells": lax.rem(mec + d, C)}, device_id_type=MESH,
        )

    def start_rs(d, _):
        rs_copy(d).start()
        return 0

    def start_b(d, _):
        b_copy(d).start()
        return 0

    def wait_rs(d, _):
        rs_copy(d).wait()
        return 0

    def wait_b(d, _):
        b_copy(d).wait()
        return 0

    lax.fori_loop(1, C, start_rs, 0)
    lax.fori_loop(1, C, start_b, 0)
    rsb[mec] = gp[mec]

    centre(1, me)
    run_ring(1, 0, min(2, HALF - 2))
    lax.fori_loop(1, C, wait_rs, 0)
    gs[...] = jnp.sum(rsb[...].astype(F32), axis=0).astype(BF16)
    sz[me] = gs[...]

    def z_copy(d):
        return pltpu.make_async_remote_copy(
            src_ref=gs, dst_ref=sz.at[me], send_sem=z_s.at[d], recv_sem=z_r.at[d],
            device_id={"runner": lax.rem(me + d, R)}, device_id_type=MESH,
        )

    def start_z(d, _):
        z_copy(d).start()
        return 0

    def wait_z(d, _):
        z_copy(d).wait()
        return 0

    lax.fori_loop(1, R, start_z, 0)
    run_ring(1, min(2, HALF - 2), min(4, HALF - 2))
    lax.fori_loop(1, R, wait_z, 0)

    def pl_copy(d):
        return pltpu.make_async_remote_copy(
            src_ref=sz, dst_ref=sb.at[mec], send_sem=pl_s.at[d], recv_sem=pl_r.at[d],
            device_id={"cells": lax.rem(chip + d, NCH) * 2 + core}, device_id_type=MESH,
        )

    def relay_copy(d):
        where = lax.rem(chip - d + NCH, NCH) * 2 + core
        return pltpu.make_async_remote_copy(
            src_ref=sb.at[where], dst_ref=sb.at[where], send_sem=rl_s.at[d], recv_sem=rl_r.at[d],
            device_id={"cells": chip * 2 + 1 - core}, device_id_type=MESH,
        )

    def start_pl(d, _):
        pl_copy(d).start()
        return 0

    def relay(d, _):
        pl_copy(d).wait_recv()
        relay_copy(d).start()
        return 0

    def sent_pl(d, _):
        pl_copy(d).wait_send()
        return 0

    def wait_relay(d, _):
        relay_copy(d).wait()
        return 0

    lax.fori_loop(1, NCH, start_pl, 0)
    sb[mec] = sz[...]
    relay_copy(0).start()
    lax.fori_loop(1, C, wait_b, 0)
    bias = jnp.sum(bsb[...], axis=0)
    run_ring(1, min(4, HALF - 2), HALF - 2)
    end_ring(1)
    lax.fori_loop(1, NCH, relay, 0)
    lax.fori_loop(0, NCH, wait_relay, 0)

    def times_gram(left):
        acc = None
        for i in range(4):
            right = jnp.concatenate([sb[i * NJ + j].reshape(16 * R, 128) for j in range(NJ)], axis=1)
            term = dot(left[:, 16 * R * i : 16 * R * (i + 1)], right)
            acc = term if acc is None else acc + term
        return acc

    trace = jnp.zeros((1, 1), F32)
    for i in range(4):
        for j in range(NJ):
            top, end = max(16 * R * i, 128 * j), min(16 * R * (i + 1), 128 * (j + 1))
            if top < end:
                block = sb[i * NJ + j].reshape(16 * R, 128)[top - 16 * R * i : end - 16 * R * i].astype(F32)
                rr = lax.broadcasted_iota(jnp.int32, block.shape, 0) + (top - 128 * j)
                cc = lax.broadcasted_iota(jnp.int32, block.shape, 1)
                part = jnp.where(rr == cc, block, 0.0)
                trace = trace + jnp.sum(jnp.sum(part, axis=0, keepdims=True), axis=1, keepdims=True)
    scaling = M / trace

    eye = qt[pl.ds(pl.multiple_of(me * SL, SL), SL), :]
    bvec = (bias * scaling).astype(BF16)
    one = times_gram(jnp.concatenate([eye, rows_of([bvec], 16)], axis=0)) * scaling
    scaled = one[0:SL].astype(BF16)
    v1 = one[SL : SL + 1]
    two = times_gram(jnp.concatenate([scaled, rows_of(list(split3(v1)), 16)], axis=0)) * scaling
    square = two[0:SL].astype(BF16)
    v2 = two[SL : SL + 1] + two[SL + 1 : SL + 2] + two[SL + 2 : SL + 3]
    three = times_gram(jnp.concatenate([square, rows_of(list(split3(v2)), 16)], axis=0)) * scaling
    cubed = three[0:SL]
    v3 = three[SL : SL + 1] + three[SL + 1 : SL + 2] + three[SL + 2 : SL + 3]
    transform = 1.0 * eye.astype(F32) - 0.5 * scaled.astype(F32) + 0.375 * square.astype(F32) - 0.3125 * cubed
    shift = bvec.astype(F32) - 0.5 * v1 + 0.375 * v2 - 0.3125 * v3
    left = jnp.concatenate([transform.astype(BF16), rows_of(list(split3(shift)), 16)], axis=0)
    left = dot_t(left, qt[...]).astype(BF16)

    finish_ring(1)

    parts = []
    for h in range(2):
        res = dot(left, ap[h])
        inc = res[SL : SL + 1] + res[SL + 1 : SL + 2] + res[SL + 2 : SL + 3]
        parts.append(res[0:SL] + (inc + mean[:, h * H : (h + 1) * H]))
    res = jnp.concatenate(parts, axis=1)
    hi = res.astype(BF16)
    lo = (res - hi.astype(F32)).astype(BF16)
    back = dot(jnp.concatenate([hi, lo], axis=0), pt[...])
    res = jnp.where(live, back[0:SL] + back[SL : 2 * SL], 0.0)
    for k in range(X):
        out[:, k, :] = res[:, k * Y : (k + 1) * Y]

    ring_sent(0)
    ring_sent(1)
    lax.fori_loop(1, NCH, sent_pl, 0)


def body(R, C, states, diffusivity, velocity, counts, obs_index, obs_value, obs_weight):
    SL, X, Y = states.shape
    CELLS = X * Y
    M = SL // 2 * R
    PAD = SL * R
    H = CELLS // 2
    fields = jnp.concatenate([diffusivity[None], velocity], axis=0)
    vm = pl.BlockSpec(memory_space=VMEM)
    hprev, hnext, fprev, fnext = pl.pallas_call(
        functools.partial(halo_kernel, C),
        out_shape=(
            jax.ShapeDtypeStruct((SL, STEPS * Y), BF16),
            jax.ShapeDtypeStruct((SL, STEPS * Y), BF16),
            jax.ShapeDtypeStruct((3, STEPS, Y), F32),
            jax.ShapeDtypeStruct((3, STEPS, Y), F32),
        ),
        in_specs=[vm, vm],
        out_specs=(vm, vm, vm, vm),
        scratch_shapes=[
            VMEM((SL, STEPS * Y), BF16), VMEM((SL, STEPS * Y), BF16),
            VMEM((3, STEPS, Y), F32), VMEM((3, STEPS, Y), F32),
            DMA((4,)), DMA((4,)),
        ],
        compiler_params=pltpu.CompilerParams(collective_id=0, has_side_effects=True),
        name="halo",
    )(states, fields)
    return pl.pallas_call(
        functools.partial(main_kernel, R, C),
        out_shape=jax.ShapeDtypeStruct((SL, X, Y), F32),
        in_specs=[vm] * 6 + [pl.BlockSpec(memory_space=pltpu.SMEM)] + [vm] * 3,
        out_specs=vm,
        scratch_shapes=[
            VMEM((5, X + 2 * STEPS, Y), F32),
            VMEM((SL, CELLS), F32),
            pltpu.SMEM((R,), jnp.int32),
            VMEM((PAD, M), BF16),
            VMEM((CELLS, CELLS), BF16),
            VMEM((R, 2, SL, H), BF16),
            VMEM((2, PAD, H), BF16),
            VMEM((R, 1, CELLS), F32),
            VMEM((C, 16, 128), BF16),
            VMEM((C, 16, 128), BF16),
            VMEM((C, 1, M), F32),
            VMEM((1, M), F32),
            VMEM((16, 128), BF16),
            VMEM((R, 16, 128), BF16),
            VMEM((C, R, 16, 128), BF16),
            DMA((R,)), DMA((R,)),
            DMA((2, 2, R // 2, 2)), DMA((2, 2, R // 2, 2)),
            DMA((C,)), DMA((C,)),
            DMA((C,)), DMA((C,)),
            DMA((R,)), DMA((R,)),
            DMA((C // 2,)), DMA((C // 2,)),
            DMA((C // 2,)), DMA((C // 2,)),
        ],
        compiler_params=pltpu.CompilerParams(
            collective_id=1, has_side_effects=True, vmem_limit_bytes=60 * 1024 * 1024
        ),
        name="cycle",
    )(
        states, hprev, hnext, fields, fprev, fnext, counts,
        obs_index.reshape(1, -1), obs_value.reshape(1, -1), obs_weight.reshape(1, -1),
    )


def solution(mesh):
    sizes = dict(mesh.shape)
    return jax.shard_map(
        functools.partial(body, sizes["runner"], sizes["cells"]),
        mesh=mesh,
        in_specs=(
            P("runner", "cells", None),
            P("cells", None),
            P(None, "cells", None),
            P(),
            P("cells"),
            P("cells"),
            P("cells"),
        ),
        out_specs=P("runner", "cells", None),
        check_vma=False,
    )
```

```python
import functools

import jax
import jax.numpy as jnp
from jax import lax
from jax.experimental import pallas as pl
from jax.experimental.pallas import tpu as pltpu
from jax.sharding import PartitionSpec as P

MESH = pl.DeviceIdType.MESH
STEPS = 4
T1, T2 = 7, 13
F32 = jnp.float32
BF16 = jnp.bfloat16
VMEM = pltpu.VMEM
DMA = pltpu.SemaphoreType.DMA


def split3(x):
    hi = x.astype(BF16)
    rest = x - hi.astype(F32)
    mid = rest.astype(BF16)
    low = (rest - mid.astype(F32)).astype(BF16)
    return hi, mid, low


def rows_of(parts, rows):
    have = sum(p.shape[0] for p in parts)
    if have < rows:
        parts = list(parts) + [jnp.zeros((rows - have, parts[0].shape[1]), parts[0].dtype)]
    return jnp.concatenate(parts, axis=0)


def dot(a, b):
    return lax.dot_general(a, b, (((1,), (0,)), ((), ())), preferred_element_type=F32)


def dot_t(a, b):
    return lax.dot_general(a, b, (((1,), (1,)), ((), ())), preferred_element_type=F32)


def main_kernel(
    R, C, NSUB,
    st_h, dif_h, vel_h, counts, idx_h, val_h, w_h,
    out,
    st, dif, vel, obs_idx, obs_val, obs_w, in_s,
    hi_s, lo_s, hprev, hnext, fhi_s, flo_s, fprev, fnext,
    cf, fc, offs, qt, pt, abuf, lmb, gp, rsb, bsb, gs, sz, sb, sf,
    level, h_s, h_r, lm_s, lm_r, ring_s, ring_r, rs_s, rs_r, b_s, b_r, z_s, z_r, pl_s, pl_r, pl_rd, rl_s, rl_r,
):
    loads = [
        pltpu.make_async_copy(src, dst, in_s.at[n])
        for n, (src, dst) in enumerate(
            ((st_h, st), (dif_h, dif), (vel_h, vel), (idx_h, obs_idx), (val_h, obs_val), (w_h, obs_w))
        )
    ]
    for load in loads:
        load.start()
    SL, X, Y = st.shape
    CELLS = X * Y
    M = SL // 2 * R
    PAD = SL * R
    H = CELLS // 2
    NJ = C // 4
    HALF = R // 2
    NCH = C // 2
    NY = 4 if NCH >= 16 else 2
    NX = NCH // NY
    OBS = obs_idx.shape[1]
    me = lax.axis_index("runner")
    mec = lax.axis_index("cells")
    core = lax.rem(mec, 2)
    chip = mec // 2
    cx = chip // NY
    cy = lax.rem(chip, NY)
    up = lax.rem(me + 1, R)
    down = lax.rem(me + R - 1, R)
    nxt = lax.rem(mec + 1, C)
    prv = lax.rem(mec + C - 1, C)

    def at(x, y):
        return (lax.rem(x + NX, NX) * NY + lax.rem(y + NY, NY)) * 2 + core

    close = [mec + 1 - 2 * core, at(cx + 1, cy), at(cx - 1, cy), at(cx, cy + 1), at(cx, cy - 1)]

    barrier = pltpu.get_barrier_semaphore()
    for who in (up, down):
        pl.semaphore_signal(barrier, inc=1, device_id={"runner": who}, device_id_type=MESH)
    for who in [nxt, prv] + close:
        pl.semaphore_signal(barrier, inc=1, device_id={"cells": who}, device_id_type=MESH)

    def tell(k):
        for who in close:
            pl.semaphore_signal(level.at[k], inc=1, device_id={"cells": who}, device_id_type=MESH)

    def hear(k):
        pl.semaphore_wait(level.at[k], 5)

    for load in loads:
        load.wait()
    for k in range(STEPS):
        cols = slice(k * Y, (k + 1) * Y)
        lo_s[:, cols] = st[:, k, :].astype(BF16)
        hi_s[:, cols] = st[:, X - STEPS + k, :].astype(BF16)
    flo_s[0] = dif[0:STEPS, :]
    fhi_s[0] = dif[X - STEPS : X, :]
    for f in range(2):
        flo_s[f + 1] = vel[f, 0:STEPS, :]
        fhi_s[f + 1] = vel[f, X - STEPS : X, :]
    pl.semaphore_wait(barrier, 9)

    halo = []
    for n, (src, dst, who) in enumerate(
        ((hi_s, hprev, nxt), (lo_s, hnext, prv), (fhi_s, fprev, nxt), (flo_s, fnext, prv))
    ):
        halo.append(
            pltpu.make_async_remote_copy(
                src_ref=src, dst_ref=dst, send_sem=h_s.at[n], recv_sem=h_r.at[n],
                device_id={"cells": who}, device_id_type=MESH,
            )
        )
    for copy in halo:
        copy.start()
    tell(0)

    total = jnp.int32(0)
    for q in range(R):
        offs[q] = total
        total = total + counts[q]
    own = counts[me]

    cell_c = lax.broadcasted_iota(jnp.int32, (CELLS, OBS), 0)
    hot = jnp.where(cell_c == obs_idx[...], 1.0, 0.0).astype(BF16)
    w = obs_w[...]
    ones = jnp.ones((1, OBS), BF16)
    x = rows_of([ones, *split3(w), *split3(w * obs_val[...])], 16)
    sums = dot_t(x, hot)
    flag = sums[0:1] > 0.5
    wsum = sums[1:2] + sums[2:3] + sums[3:4]
    vsum = sums[4:5] + sums[5:6] + sums[6:7]
    r_i = lax.broadcasted_iota(jnp.int32, (CELLS, CELLS), 0)
    c_i = lax.broadcasted_iota(jnp.int32, (CELLS, CELLS), 1)
    upper = jnp.where(r_i < c_i, 1.0, 0.0).astype(BF16)
    flags = jnp.where(flag, 1.0, 0.0)
    before = dot(rows_of([flags.astype(BF16)], 16), upper)[0:1]
    n_obs = jnp.sum(flags, axis=1, keepdims=True)
    cell_r = lax.broadcasted_iota(jnp.int32, (1, CELLS), 1).astype(F32)
    place = jnp.where(flag, before, n_obs + cell_r - before).astype(jnp.int32)
    pt[...] = jnp.where(r_i == place, 1.0, 0.0).astype(BF16)

    hear(0)
    tell(1)
    for copy in halo:
        copy.wait()

    for k in range(X + 2 * STEPS):
        if k < STEPS:
            d, v0, v1 = (fprev[f, k : k + 1, :] for f in range(3))
        elif k < STEPS + X:
            d = dif[k - STEPS : k - STEPS + 1, :]
            v0, v1 = (vel[f, k - STEPS : k - STEPS + 1, :] for f in range(2))
        else:
            d, v0, v1 = (fnext[f, k - STEPS - X : k - STEPS - X + 1, :] for f in range(3))
        cf[0, k : k + 1, :] = d - 0.5 * v0
        cf[1, k : k + 1, :] = d + 0.5 * v0
        cf[2, k : k + 1, :] = d - 0.5 * v1
        cf[3, k : k + 1, :] = d + 0.5 * v1
        cf[4, k : k + 1, :] = 1.0 - 4.0 * d

    def march(g, _):
        sl = pl.ds(pl.multiple_of(g * 16, 16), 16)
        u = [hprev[sl, k * Y : (k + 1) * Y].astype(F32) for k in range(STEPS)]
        u += [st[sl, k, :] for k in range(X)]
        u += [hnext[sl, k * Y : (k + 1) * Y].astype(F32) for k in range(STEPS)]
        for step in range(STEPS):
            new = []
            for k in range(1, len(u) - 1):
                row = k + step
                c = u[k]
                right = pltpu.roll(c, Y - 1, 1)
                left = pltpu.roll(c, 1, 1)
                acc = cf[0, row : row + 1, :] * u[k + 1] + cf[1, row : row + 1, :] * u[k - 1]
                acc = acc + cf[2, row : row + 1, :] * right + cf[3, row : row + 1, :] * left
                acc = acc + c * (cf[4, row : row + 1, :] - 0.05 * (c * c))
                new.append(acc)
            u = new
        for k in range(X):
            fc[sl, k * Y : (k + 1) * Y] = u[k]
        return 0

    lax.fori_loop(0, SL // 16, march, 0)

    slot = lax.broadcasted_iota(jnp.int32, (SL, 1), 0)
    live = slot < own
    lsum = jnp.sum(jnp.where(live, fc[...], 0.0), axis=0, keepdims=True)
    lmean = lsum / own.astype(F32)
    local = jnp.where(live, fc[...] - lmean, 0.0).astype(BF16)
    moved = dot_t(local, pt[...]).astype(BF16)
    abuf[0, me] = moved[:, :H]
    abuf[1, me] = moved[:, H:]
    rows3 = rows_of([*split3(lmean), *split3(wsum), *split3(vsum)], 16)
    rows3 = dot_t(rows3, pt[...])
    lmb[me] = rows3[0:1] + rows3[1:2] + rows3[2:3]
    wperm = (rows3[3:4] + rows3[4:5] + rows3[5:6])[:, :H]
    vperm = (rows3[6:7] + rows3[7:8] + rows3[8:9])[:, :H]

    SUB = SL // NSUB
    LOW, HIGH = range(NSUB // 2), range(NSUB // 2, NSUB)

    def each(first, last, what):
        def go(d, _):
            what(d)
            return 0

        lax.fori_loop(first, last, go, 0)

    def ring_copy(h, s, way, sub):
        owner = lax.rem(me - s + R, R) if way == 0 else lax.rem(me + s, R)
        part = abuf.at[h, owner, pl.ds(pl.multiple_of(sub * SUB, SUB), SUB)]
        return pltpu.make_async_remote_copy(
            src_ref=part, dst_ref=part, send_sem=ring_s.at[h], recv_sem=ring_r.at[way, h, s, sub],
            device_id={"runner": up if way == 0 else down}, device_id_type=MESH,
        )

    def lm_copy(s, way):
        owner = lax.rem(me - s + R, R) if way == 0 else lax.rem(me + s, R)
        return pltpu.make_async_remote_copy(
            src_ref=lmb.at[owner], dst_ref=lmb.at[owner], send_sem=lm_s, recv_sem=lm_r.at[way, s],
            device_id={"runner": up if way == 0 else down}, device_id_type=MESH,
        )

    def ring_start(h):
        for sub in range(NSUB):
            for way in range(2):
                ring_copy(h, 0, way, sub).start()

    def sub_step(h, s, sub):
        for way in range(2):
            ring_copy(h, s, way, sub).wait_recv()
            ring_copy(h, s + 1, way, sub).start()

    STEPS_H = (HALF - 2) * NSUB

    def ring_run(h, first, last):
        def one(t, _):
            sub_step(h, t // NSUB, lax.rem(t, NSUB))
            return 0

        if last > first:
            lax.fori_loop(first, last, one, 0)

    def ring_tail(h):
        for sub in range(NSUB):
            for way in range(2):
                ring_copy(h, HALF - 2, way, sub).wait_recv()
                if sub in (LOW, HIGH)[way]:
                    ring_copy(h, HALF - 1, way, sub).start()

    def ring_end(h):
        for way in range(2):
            for sub in (LOW, HIGH)[way]:
                ring_copy(h, HALF - 1, way, sub).wait_recv()

    def landed(ref, sem):
        pltpu.make_async_copy(ref, ref, sem).wait()

    for way in range(2):
        lm_copy(0, way).start()
    ring_start(0)
    hear(1)
    tell(2)

    slots = lax.broadcasted_iota(jnp.int32, (SL, M), 0)
    mems = lax.broadcasted_iota(jnp.int32, (SL, M), 1)

    def build(q):
        hit = (mems == slots + offs[q]) & (slots < counts[q])
        qt[pl.ds(pl.multiple_of(q * SL, SL), SL), :] = jnp.where(hit, 1.0, 0.0).astype(BF16)

    PER = R // max(HALF - 2, 1)

    def first_ring(s, early):
        for way in range(2):
            lm_copy(s, way).wait_recv()
            lm_copy(s + 1, way).start()
        for sub in range(NSUB):
            sub_step(0, s, sub)
        early(s)
        build(2 * s)
        build(2 * s + 1)

    def early_start(s):
        for way in range(2):
            ring_copy(1, 0, way, s).start()

    each(0, NSUB, lambda s: first_ring(s, early_start))
    each(NSUB, HALF - 2, lambda s: first_ring(s, lambda t: sub_step(1, 0, t - NSUB)))
    t0 = HALF - 2 - NSUB
    hear(2)
    tell(3)
    for way in range(2):
        lm_copy(HALF - 2, way).wait_recv()
    lm_copy(HALF - 1, 0).start()
    ring_tail(0)
    sub_step(1, 0, t0)
    for q in range(2 * (HALF - 2), R):
        build(q)
    p_i = lax.broadcasted_iota(jnp.int32, (64, SL), 0)
    l_i = lax.broadcasted_iota(jnp.int32, (64, SL), 1)
    wanted = (p_i >> 4) * (16 * R) + 16 * me + (p_i & 15)
    pick = []
    for q in range(R):
        hit = (wanted == l_i + offs[q]) & (l_i < counts[q])
        pick.append(jnp.where(hit, 1.0, 0.0).astype(BF16))
    pick = jnp.concatenate(pick, axis=1)
    hear(3)
    lm_copy(HALF - 1, 0).wait_recv()
    mean = jnp.zeros((1, CELLS), F32)
    for q in range(R):
        mean = mean + counts[q].astype(F32) * lmb[q]
    mean = mean / M
    shifts = jnp.concatenate([lmb[q] - mean for q in range(R)], axis=0)
    ring_end(0)

    first_half = abuf[0].reshape(PAD, H)
    shift0 = shifts[:, :H]
    rows_a = dot(pick, first_half)
    want = wanted[:, 0:1]
    for q in range(R):
        mine = (want >= offs[q]) & (want < offs[q] + counts[q])
        rows_a = rows_a + jnp.where(mine, shift0[q : q + 1], 0.0)
    weighted = (rows_a * wperm).astype(BF16)
    grad = vperm - wperm * mean[:, :H]
    left = jnp.concatenate([weighted, rows_of(list(split3(grad)), 16)], axis=0)
    wide = dot_t(left, first_half)
    extra = [dot_t(left, part) for part in split3(shift0)]
    extra = extra[0] + extra[1] + extra[2]
    wide = jnp.concatenate([wide[:, q * SL : (q + 1) * SL] + extra[:, q : q + 1] for q in range(R)], axis=1)
    wide_hi = wide.astype(BF16)
    wide_lo = (wide - wide_hi.astype(F32)).astype(BF16)
    both = dot(jnp.concatenate([wide_hi, wide_lo], axis=0), qt[...])
    gram = both[0:80] + both[80:160]
    for c in range(C):
        i, j = c // NJ, c % NJ
        gp[c] = gram[16 * i : 16 * i + 16, 128 * j : 128 * j + 128].astype(BF16)
    bsb[mec] = gram[64:65] + gram[65:66] + gram[66:67]

    def rs_copy(d):
        to = lax.rem(mec + d, C)
        return pltpu.make_async_remote_copy(
            src_ref=gp.at[to], dst_ref=rsb.at[mec], send_sem=rs_s, recv_sem=rs_r,
            device_id={"cells": to}, device_id_type=MESH,
        )

    def b_copy(d):
        return pltpu.make_async_remote_copy(
            src_ref=bsb.at[mec], dst_ref=bsb.at[mec], send_sem=b_s, recv_sem=b_r,
            device_id={"cells": lax.rem(mec + d, C)}, device_id_type=MESH,
        )

    def z_copy(d):
        return pltpu.make_async_remote_copy(
            src_ref=gs, dst_ref=sz.at[me], send_sem=z_s, recv_sem=z_r,
            device_id={"runner": lax.rem(me + d, R)}, device_id_type=MESH,
        )

    diagonal = cx == cy
    piece = jnp.where(cx > cy, 1 - core, core)

    def pl_copy(d, second):
        which = 1 - piece if second else piece
        sem = pl_rd.at[cx] if second else pl_r.at[d]
        return pltpu.make_async_remote_copy(
            src_ref=sz.at[pl.ds(which * (R // 2), R // 2)], dst_ref=sb.at[mec * 2 + which],
            send_sem=pl_s.at[1 if second else 0], recv_sem=sem,
            device_id={"cells": lax.rem(chip + d, NCH) * 2 + core}, device_id_type=MESH,
        )

    def relay_copy(where):
        return pltpu.make_async_remote_copy(
            src_ref=sb.at[where], dst_ref=sb.at[where], send_sem=rl_s, recv_sem=rl_r,
            device_id={"cells": chip * 2 + 1 - core}, device_id_type=MESH,
        )

    def first_piece(who):
        wx, wy = who // NY, lax.rem(who, NY)
        return (who * 2 + core) * 2 + jnp.where(wx > wy, 1 - core, core)

    def second_piece(n):
        return ((n * NY + n) * 2 + core) * 2 + 1 - core

    each(1, C, lambda d: rs_copy(d).start())
    rsb[mec] = gp[mec]
    each(1, C, lambda d: b_copy(d).start())

    t1, t2 = T1, T2
    ring_run(1, t0 + 1, t1)
    landed(rsb.at[pl.ds(0, C - 1)], rs_r)
    gs[...] = jnp.sum(rsb[...].astype(F32), axis=0).astype(BF16)
    sz[me] = gs[...]
    each(1, R, lambda d: z_copy(d).start())
    ring_run(1, t1, t2)
    landed(sz.at[pl.ds(0, R - 1)], z_r)

    each(1, NCH, lambda d: pl_copy(d, False).start())

    @pl.when(diagonal)
    def _():
        each(1, NCH, lambda d: pl_copy(d, True).start())

    sb[mec * 2] = sz[0 : R // 2]
    sb[mec * 2 + 1] = sz[R // 2 : R]
    relay_copy(first_piece(chip)).start()

    @pl.when(diagonal)
    def _():
        relay_copy(second_piece(cx)).start()

    landed(bsb.at[pl.ds(0, C - 1)], b_r)
    bias = jnp.sum(bsb[...], axis=0)
    ring_run(1, t2, STEPS_H)
    ring_tail(1)

    def relay(d):
        pltpu.make_async_copy(sb.at[0], sb.at[0], pl_r.at[d]).wait()
        relay_copy(first_piece(lax.rem(chip - d + NCH, NCH))).start()

    each(1, NCH, relay)
    for n in range(NX):

        @pl.when(chip != n * NY + n)
        def _():
            landed(sb.at[0], pl_rd.at[n])
            relay_copy(second_piece(n)).start()

    landed(sb.at[pl.ds(0, NCH + NX)], rl_r)

    def part(x, y, k, half):
        return sb[((x * NY + y) * 2 + k) * 2 + half].reshape(128, 128)

    for x in range(NX):
        sf[256 * x : 256 * x + 128, 256 * x : 256 * x + 128] = part(x, x, 0, 0)
        sf[256 * x + 128 : 256 * x + 256, 256 * x : 256 * x + 128] = part(x, x, 0, 1)
        sf[256 * x : 256 * x + 128, 256 * x + 128 : 256 * x + 256] = part(x, x, 1, 0)
        sf[256 * x + 128 : 256 * x + 256, 256 * x + 128 : 256 * x + 256] = part(x, x, 1, 1)
        for y in range(x + 1, NY):
            for k, half, value in (
                (0, 0, part(x, y, 0, 0)),
                (1, 1, part(x, y, 1, 1)),
            ):
                sf[256 * x + 128 * half : 256 * x + 128 * half + 128, 256 * y + 128 * k : 256 * y + 128 * k + 128] = value
                sf[256 * y + 128 * k : 256 * y + 128 * k + 128, 256 * x + 128 * half : 256 * x + 128 * half + 128] = value.T
            for k, half, value in (
                (0, 1, part(y, x, 0, 1)),
                (1, 0, part(y, x, 1, 0)),
            ):
                sf[256 * y + 128 * half : 256 * y + 128 * half + 128, 256 * x + 128 * k : 256 * x + 128 * k + 128] = value
                sf[256 * x + 128 * k : 256 * x + 128 * k + 128, 256 * y + 128 * half : 256 * y + 128 * half + 128] = value.T

    def times_gram(left):
        return dot(left, sf[...])

    rr = lax.broadcasted_iota(jnp.int32, (128, 128), 0)
    cc = lax.broadcasted_iota(jnp.int32, (128, 128), 1)
    trace = jnp.zeros((1, 128), F32)
    for x in range(NX):
        for k in range(2):
            trace = trace + jnp.sum(jnp.where(rr == cc, part(x, x, k, k).astype(F32), 0.0), axis=0, keepdims=True)
    trace = jnp.sum(trace, axis=1, keepdims=True)
    scaling = M / trace

    eye = qt[pl.ds(pl.multiple_of(me * SL, SL), SL), :]
    bvec = (bias * scaling).astype(BF16)
    one = times_gram(jnp.concatenate([eye, rows_of([bvec], 16)], axis=0)) * scaling
    scaled = one[0:SL].astype(BF16)
    v1 = one[SL : SL + 1]
    two = times_gram(jnp.concatenate([scaled, rows_of(list(split3(v1)), 16)], axis=0)) * scaling
    square = two[0:SL].astype(BF16)
    v2 = two[SL : SL + 1] + two[SL + 1 : SL + 2] + two[SL + 2 : SL + 3]
    three = times_gram(jnp.concatenate([square, rows_of(list(split3(v2)), 16)], axis=0)) * scaling
    cubed = three[0:SL]
    v3 = three[SL : SL + 1] + three[SL + 1 : SL + 2] + three[SL + 2 : SL + 3]
    transform = 1.0 * eye.astype(F32) - 0.5 * scaled.astype(F32) + 0.375 * square.astype(F32) - 0.3125 * cubed
    shift = bvec.astype(F32) - 0.5 * v1 + 0.375 * v2 - 0.3125 * v3
    left = jnp.concatenate([transform.astype(BF16), rows_of(list(split3(shift)), 16)], axis=0)
    mem_r = lax.broadcasted_iota(jnp.int32, (1, M), 1)
    owner = [(mem_r >= offs[q]) & (mem_r < offs[q] + counts[q]) for q in range(R)]
    owner = jnp.concatenate([jnp.where(o, 1.0, 0.0) for o in owner], axis=0).astype(BF16)
    per_runner = dot_t(left, owner)
    moves = lax.dot_general(
        per_runner, shifts, (((1,), (0,)), ((), ())),
        precision=lax.Precision.HIGHEST, preferred_element_type=F32,
    )
    left = dot_t(left, qt[...]).astype(BF16)

    ring_end(1)

    parts = []
    for h in range(2):
        res = dot(left, abuf[h].reshape(PAD, H)) + moves[:, h * H : (h + 1) * H]
        inc = res[SL : SL + 1] + res[SL + 1 : SL + 2] + res[SL + 2 : SL + 3]
        parts.append(res[0:SL] + (inc + mean[:, h * H : (h + 1) * H]))
    res = jnp.concatenate(parts, axis=1)
    hi = res.astype(BF16)
    lo = (res - hi.astype(F32)).astype(BF16)
    back = dot(jnp.concatenate([hi, lo], axis=0), pt[...])
    res = jnp.where(live, back[0:SL] + back[SL : 2 * SL], 0.0)
    for k in range(X):
        out[:, k, :] = res[:, k * Y : (k + 1) * Y]

    for h in range(2):
        landed(abuf.at[h, pl.ds(0, R - 1)], ring_s.at[h])
    landed(lmb.at[pl.ds(0, R - 1)], lm_s)
    landed(gp.at[pl.ds(0, C - 1)], rs_s)
    landed(bsb.at[pl.ds(0, C - 1)], b_s)
    landed(sz.at[pl.ds(0, R - 1)], z_s)
    landed(sb.at[pl.ds(0, NCH - 1)], pl_s.at[0])

    @pl.when(diagonal)
    def _():
        landed(sb.at[pl.ds(0, NCH - 1)], pl_s.at[1])

    landed(sb.at[pl.ds(0, NCH + NX)], rl_s)


def body(R, C, states, diffusivity, velocity, counts, obs_index, obs_value, obs_weight):
    SL, X, Y = states.shape
    CELLS = X * Y
    M = SL // 2 * R
    PAD = SL * R
    H = CELLS // 2
    NSUB = 4
    vm = pl.BlockSpec(memory_space=VMEM)
    hbm = pl.BlockSpec(memory_space=pltpu.HBM)
    n_obs = obs_index.shape[0]
    return pl.pallas_call(
        functools.partial(main_kernel, R, C, NSUB),
        out_shape=jax.ShapeDtypeStruct((SL, X, Y), F32),
        in_specs=[hbm] * 3 + [pl.BlockSpec(memory_space=pltpu.SMEM)] + [hbm] * 3,
        out_specs=vm,
        scratch_shapes=[
            VMEM((SL, X, Y), F32), VMEM((X, Y), F32), VMEM((2, X, Y), F32),
            VMEM((1, n_obs), jnp.int32), VMEM((1, n_obs), F32), VMEM((1, n_obs), F32),
            DMA((6,)),
            VMEM((SL, STEPS * Y), BF16), VMEM((SL, STEPS * Y), BF16),
            VMEM((SL, STEPS * Y), BF16), VMEM((SL, STEPS * Y), BF16),
            VMEM((3, STEPS, Y), F32), VMEM((3, STEPS, Y), F32),
            VMEM((3, STEPS, Y), F32), VMEM((3, STEPS, Y), F32),
            VMEM((5, X + 2 * STEPS, Y), F32),
            VMEM((SL, CELLS), F32),
            pltpu.SMEM((R,), jnp.int32),
            VMEM((PAD, M), BF16),
            VMEM((CELLS, CELLS), BF16),
            VMEM((2, R, SL, H), BF16),
            VMEM((R, 1, CELLS), F32),
            VMEM((C, 16, 128), BF16),
            VMEM((C, 16, 128), BF16),
            VMEM((C, 1, M), F32),
            VMEM((16, 128), BF16),
            VMEM((R, 16, 128), BF16),
            VMEM((2 * C, R // 2, 16, 128), BF16),
            VMEM((M, M), BF16),
            pltpu.SemaphoreType.REGULAR((4,)),
            DMA((4,)), DMA((4,)),
            DMA, DMA((2, R // 2)),
            DMA((2,)), DMA((2, 2, R // 2, NSUB)),
            DMA, DMA, DMA, DMA, DMA, DMA,
            DMA((2,)), DMA((C // 2,)), DMA((4,)),
            DMA, DMA,
        ],
        compiler_params=pltpu.CompilerParams(
            collective_id=1, has_side_effects=True, vmem_limit_bytes=60 * 1024 * 1024
        ),
        name="cycle",
    )(
        states, diffusivity, velocity, counts,
        obs_index.reshape(1, -1), obs_value.reshape(1, -1), obs_weight.reshape(1, -1),
    )


def solution(mesh):
    sizes = dict(mesh.shape)
    return jax.shard_map(
        functools.partial(body, sizes["runner"], sizes["cells"]),
        mesh=mesh,
        in_specs=(
            P("runner", "cells", None),
            P("cells", None),
            P(None, "cells", None),
            P(),
            P("cells"),
            P("cells"),
            P("cells"),
        ),
        out_specs=P("runner", "cells", None),
        check_vma=False,
    )
```
